32 devices in a mesh: gz: 32 (over z, y, x, core).
Axes of the slice: x: 2, y: 2, z: 4, core: 2. Of those that a mesh axis runs over, the one named last changes fastest.
Arguments:
- velocity: float32 [3, 128, 256, 512], P(None, 'gz'), may hold values from -0.3 to 0.3
- offsets: float32 [3, 16384], P(None, 'gz'), may hold values from 1.2 to 1.8
- bases: int32 [3, 16384], P(None, 'gz'), may hold values from 0 to 511, as said below
- targets: float32 [3, 16384], P(None, 'gz'), may hold values from 1 to 2
- stiffness: float32 [16384], P('gz'), may hold values from 10 to 100
- active_block_count: int32 [32], P('gz'), may hold values from 1 to 2, as said below
Outputs:
- velocity_out: float32 [3, 128, 256, 512], P(None, 'gz')
- offsets_out: float32 [3, 16384], P(None, 'gz')
The draws below stay inside these ranges and needn't reach their ends.
Inputs may be any that keep to these rules, and one draw needn't show every extreme that they name: `bases`: rows are x, y, z. x lies in 0..511 and y in 0..255; the z of marker m lies in the slab of index m // 512, from (m // 512) * 4 to (m // 512) * 4 + 3. `active_block_count`: in every draw some slab uses all 2 blocks.
All inputs are finite; a program needn't handle non-finite values.
Results may differ from the reference program's by a relative error of at most 0.0015.
Values may be sent and summed in bfloat16 or wider, within the bound.
A program may use at most 192 MiB of HBM per device.

```python
import math
import jax
import jax.numpy as jnp
from jax import lax

NX = 512
NY = 256
CZ = 4
M_DEV = 512
BLK = 256
STEPS = 2
NBLK = 2
NZ = 128
MARKERS = 16384
SLABS = 32


def draw_bases(key, part):
    first_key, second_key, third_key = jax.random.split(key, 3)
    x_cells = jax.random.randint(first_key, (MARKERS,), 0, NX)
    y_cells = jax.random.randint(second_key, (MARKERS,), 0, NY)
    owners = jnp.arange(MARKERS, dtype=jnp.int32) // M_DEV
    z_cells = owners * CZ + jax.random.randint(third_key, (MARKERS,), 0, CZ)
    return jnp.stack([x_cells, y_cells, z_cells]).astype(jnp.int32)


def draw_active_block_count(key, part):
    count_key, chosen_key = jax.random.split(key)
    counts = jax.random.randint(count_key, (SLABS,), 1, NBLK + 1)
    chosen = jax.random.randint(chosen_key, (), 0, SLABS)
    return counts.at[chosen].set(NBLK).astype(jnp.int32)


def block_levels(own_key, extent, cuts, low, largest):
    def one(dim, parts):
        heights = jax.random.uniform(jax.random.fold_in(jax.random.fold_in(own_key, 6), dim), (parts,), jnp.float32, low / len(cuts), largest / len(cuts))
        return jnp.repeat(jnp.exp(heights), extent[dim] // parts).reshape((-1,) + (1,) * (len(extent) - dim - 1))

    level = one(*cuts[0])
    for cut in cuts[1:]:
        level = level * one(*cut)
    return level


def bell_draw(own_key, extent, width, bound, pieces=(), held_as=jnp.bfloat16):
    drawn = jax.random.normal(own_key, extent, jnp.float32) * width
    if len(pieces) > 0:
        drawn = block_levels(own_key, extent, pieces, -0.22, 0.18) * drawn
    return jnp.clip(drawn, min=-bound, max=bound).astype(held_as)


def setup_inputs(seed: int = 0) -> dict:
    keys = jax.random.split(jax.random.key(seed), 7)
    return {
        "velocity": bell_draw(keys[0], (3, NZ, NY, NX), 0.1, 0.3, ((1, 32),), jnp.float32),
        "offsets": jnp.clip(1.2 + 0.5999999 * jax.random.uniform(keys[1], (3, MARKERS), jnp.float32) ** block_levels(keys[1], (3, MARKERS), ((1, 32),), -0.2, 0.2), 1.2, 1.8),
        "bases": draw_bases(jax.random.fold_in(keys[6], 71), 0),
        "targets": jnp.clip(1.0 + 1.0 * jax.random.uniform(keys[3], (3, MARKERS), jnp.float32) ** block_levels(keys[3], (3, MARKERS), ((1, 32),), -0.2, 0.2), 1.0, 2.0),
        "stiffness": jnp.clip(jnp.exp(math.log(100.0) - 2.3025851 * jax.random.uniform(keys[4], (MARKERS,), jnp.float32) ** block_levels(keys[4], (MARKERS,), ((0, 32),), -0.2, 0.2)), 10.0, 100.0),
        "active_block_count": draw_active_block_count(jax.random.fold_in(keys[6], 71), 0),
    }


def kernel(offsets):
    steps_back = jnp.arange(4).astype(jnp.float32)
    return 0.25 * (1.0 + jnp.cos((0.5 * math.pi) * (offsets[:, None, :] - steps_back[None, :, None])))


def advance(velocity, forcing):
    laplace = -6.0 * velocity
    transport_velocity = jnp.zeros_like(velocity)
    for sweep_sense in (1, 2, 3):
        upper_cells = jnp.roll(velocity, -1, sweep_sense)
        lower_cells = jnp.roll(velocity, 1, sweep_sense)
        transfer_buffer = 3 - sweep_sense
        laplace = laplace + upper_cells + lower_cells
        transport_velocity = transport_velocity + velocity[transfer_buffer][None] * (upper_cells - lower_cells) * 0.5
    return velocity + 0.2 * (0.3 * laplace - transport_velocity + forcing)


def rounded(values):
    return lax.optimization_barrier(values.astype(jnp.bfloat16)).astype(jnp.float32)


def reference(velocity, offsets, bases, targets, stiffness, active_block_count):
    markers = offsets.shape[1]
    ordinal = jnp.arange(markers, dtype=jnp.int32)
    living = ((ordinal % M_DEV) // BLK < active_block_count[ordinal // M_DEV]).astype(jnp.float32)
    reach = jnp.arange(4, dtype=jnp.int32)
    xcells = (bases[0][None, :] + reach[:, None]) % NX
    ycells = (bases[1][None, :] + reach[:, None]) % NY
    zcells = (bases[2][None, :] + reach[:, None]) % NZ
    shape_all = (4, 4, 4, markers)
    z_index = jnp.broadcast_to(zcells[:, None, None, :], shape_all).reshape(-1)
    y_index = jnp.broadcast_to(ycells[None, :, None, :], shape_all).reshape(-1)
    x_index = jnp.broadcast_to(xcells[None, None, :, :], shape_all).reshape(-1)
    for step_number in range(STEPS):
        weights = kernel(offsets)
        forces = living[None, :] * stiffness[None, :] * (targets - offsets)
        vertical = rounded((forces[:, None, None, :] * weights[2][None, :, None, :]) * weights[1][None, None, :, :])
        across = rounded(weights[0])
        amounts = vertical[:, :, :, None, :] * across[None, None, None, :, :]
        forcing = jnp.zeros_like(velocity).at[:, z_index, y_index, x_index].add(amounts.reshape(3, -1))
        velocity = advance(velocity, forcing)
        lowered = velocity.astype(jnp.bfloat16)
        picked = lowered[:, z_index, y_index, x_index].astype(jnp.float32).reshape(3, 4, 4, 4, markers)
        mixed = rounded(weights[2][:, None, :] * weights[1][None, :, :])
        sampled = jnp.sum((mixed[None, :, :, None, :] * picked) * weights[0][None, None, None, :, :], axis=(1, 2, 3))
        offsets = offsets + 0.2 * (living[None, :] * sampled)
    return velocity, offsets
```

```python
import functools
import math

import jax
import jax.numpy as jnp
from jax import lax
from jax.experimental import pallas as pl
from jax.experimental.pallas import tpu as pltpu
from jax.sharding import PartitionSpec as P

BLK = 256
STEPS = 2
DT = 0.2
VISC = 0.3
LANES = 128
PAD = 8
CHUNKS = 8
MESH = pl.DeviceIdType.MESH


def weights_of(offsets):
    angle = (0.5 * math.pi) * offsets
    c, s = jnp.cos(angle), jnp.sin(angle)
    return [0.25 * (1.0 + c), 0.25 * (1.0 + s), 0.25 * (1.0 - c), 0.25 * (1.0 - s)]


def banded(across, cell, weights, extent):
    apart = across - cell
    if extent & (extent - 1) == 0:
        apart = apart & (extent - 1)
    else:
        apart = jnp.where(apart < 0, apart + extent, apart)
    table = jnp.where(apart == 3, weights[3], 0.0)
    for j in (2, 1, 0):
        table = jnp.where(apart == j, weights[j], table)
    return table


def plane_weights(level, weights_z, layers):
    planes = []
    for z in range(layers):
        row = jnp.zeros(level.shape, jnp.float32)
        for j in range(4):
            row = jnp.where(level + j == z, weights_z[j], row)
        planes.append(row)
    return planes


def columns_of(rows):
    pad = -len(rows) % 8
    zero = jnp.zeros_like(rows[0])
    return jnp.concatenate(rows + [zero] * pad, axis=0).T


def kernel(
    v_hbm, off_ref, base_ref, tgt_ref, stiff_ref, cnt_ref,
    out_ref, offout_ref,
    vv, own, near, send, halo, low, lhs, xtab, xtab32, ytab, slhs, col, rowg, acc,
    partbuf, partin, in_sem, mk_sem, hs_sem, hr_sem, ps_sem, pr_sem,
):
    _, _, layers, nxb, nyp, _ = vv.shape
    ny = nyp - 2 * PAD
    nx = nxb * LANES
    markers = off_ref.shape[1]
    both = 2 * markers
    rows = ny // CHUNKS
    me = lax.axis_index("gz")
    count = lax.axis_size("gz")
    right = lax.rem(me + 1, count)
    left = lax.rem(me + count - 1, count)
    edges = (0, layers - 1)
    inner = tuple(range(1, layers - 1))
    order = inner + edges
    place = {z: i for i, z in enumerate(order)}

    barrier = pltpu.get_barrier_semaphore()
    for neighbour in (left, right):
        pl.semaphore_signal(barrier, inc=1, device_id=(neighbour,), device_id_type=MESH)

    def load(z, b):
        return pltpu.make_async_copy(
            v_hbm.at[:, z, :, pl.ds(b * LANES, LANES)],
            vv.at[0, :, z, b, pl.ds(PAD, ny), :],
            in_sem.at[z, b],
        )

    for z in edges + inner:
        for b in range(nxb):
            load(z, b).start()

    living = (
        lax.broadcasted_iota(jnp.int32, (1, markers), 1) // BLK < cnt_ref[0]
    ).astype(jnp.float32)
    own[0:3, :] = off_ref[...]
    own[3:5, :] = base_ref[0:2, :].astype(jnp.float32)
    own[5:6, :] = (base_ref[2:3, :] - me * layers).astype(jnp.float32)
    own[6:9, :] = tgt_ref[...]
    own[9:10, :] = living
    own[10:11, :] = living * stiff_ref[...]
    own[11:16, :] = jnp.zeros((5, markers), jnp.float32)

    pl.semaphore_wait(barrier, 2)
    marker_copy = pltpu.make_async_remote_copy(
        own, near, mk_sem.at[0], mk_sem.at[1], device_id=(right,), device_id_type=MESH
    )
    marker_copy.start()

    def halo_copy(step, side, k):
        r = pl.ds(k * rows, rows)
        if step == 0:
            source = send.at[side, :, r]
        else:
            source = low.at[:, pl.ds(place[edges[side]] * ny + k * rows, rows)]
        return pltpu.make_async_remote_copy(
            source,
            halo.at[step, 1 - side, :, r],
            hs_sem.at[step, side, k],
            hr_sem.at[step, 1 - side, k],
            device_id=((left, right)[side],),
            device_id_type=MESH,
        )

    for z in edges:
        for b in range(nxb):
            load(z, b).wait()

    def cast_chunk(k, _):
        for side, z in enumerate(edges):
            for c in range(3):
                for b in range(nxb):
                    send[side, c, pl.ds(k * rows, rows), b * LANES : (b + 1) * LANES] = vv[
                        0, c, z, b, pl.ds(PAD + k * rows, rows), :
                    ].astype(jnp.bfloat16)
        for side in range(2):
            halo_copy(0, side, k).start()
        return 0

    lax.fori_loop(0, CHUNKS, cast_chunk, 0)
    for z in inner:
        for b in range(nxb):
            load(z, b).wait()

    def wrap_rows(now):
        for c in range(3):
            for z in range(layers):
                for b in range(nxb):
                    vv[now, c, z, b, PAD - 1 : PAD, :] = vv[now, c, z, b, PAD + ny - 1 : PAD + ny, :]
                    vv[now, c, z, b, PAD + ny : PAD + ny + 1, :] = vv[now, c, z, b, PAD : PAD + 1, :]

    def stencil(now, z, n=8, unroll=2):
        lane = lax.broadcasted_iota(jnp.int32, (n, LANES), 1)
        first, last = lane == 0, lane == LANES - 1
        new = 1 - now

        def body(i, _):
            y0 = PAD + i * n
            here = [[vv[now, c, z, b, pl.ds(y0, n), :] for b in range(nxb)] for c in range(3)]
            fore = [[pltpu.roll(h, LANES - 1, 1) for h in hs] for hs in here]
            back = [[pltpu.roll(h, 1, 1) for h in hs] for hs in here]
            for b in range(nxb):
                up = [DT * VISC - (0.5 * DT) * here[c][b] for c in range(3)]
                down = [DT * VISC + (0.5 * DT) * here[c][b] for c in range(3)]
                for c in range(3):
                    total = (1.0 - 6.0 * DT * VISC) * here[c][b]
                    total += up[1] * vv[now, c, z, b, pl.ds(y0 + 1, n), :]
                    total += down[1] * vv[now, c, z, b, pl.ds(y0 - 1, n), :]
                    if z < layers - 1:
                        total += up[2] * vv[now, c, z + 1, b, pl.ds(y0, n), :]
                    if z > 0:
                        total += down[2] * vv[now, c, z - 1, b, pl.ds(y0, n), :]
                    total += up[0] * jnp.where(last, fore[c][(b + 1) % nxb], fore[c][b])
                    total += down[0] * jnp.where(first, back[c][(b - 1) % nxb], back[c][b])
                    vv[new, c, z, b, pl.ds(y0, n), :] = total
            return 0

        lax.fori_loop(0, ny // n, body, 0, unroll=unroll)

    def tables(step):
        halves = []
        for i, ref in enumerate((own, near)):
            info = ref[...]
            offsets = info[0:3]
            if step > 0:
                if i == 0:
                    moved = partbuf[step - 1, 0, 0:3, :] + partin[step - 1, 1, 0:3, :]
                else:
                    moved = partin[step - 1, 0, 0:3, :] + partbuf[step - 1, 1, 0:3, :]
                offsets = offsets + DT * (info[9:10] * moved)
                ref[0:3, :] = offsets
            level = info[5:6] - float(i * layers)
            forces = info[10:11] * (info[6:9] - offsets)
            halves.append((offsets, info[3:5].astype(jnp.int32), level.astype(jnp.int32), forces))
        offsets, cells, level, forces = [jnp.concatenate(p, axis=1) for p in zip(*halves)]
        weights = weights_of(offsets)
        planes = plane_weights(level, [w[2:3] for w in weights], layers)
        lines = []
        for a in range(2):
            lines += [cells[a : a + 1].astype(jnp.float32)] + [w[a : a + 1] for w in weights]
        col[...] = columns_of(lines + planes)
        for z in range(layers):
            for c in range(3):
                rowg[z, c : c + 1, :] = forces[c : c + 1] * planes[z]
        wy = [w[1:2] for w in weights]

        def ybody(i, _):
            across = lax.broadcasted_iota(jnp.int32, (32, both), 0) + i * 32
            ytab[pl.ds(i * 32, 32), :] = banded(across, cells[1:2], wy, ny)
            return 0

        lax.fori_loop(0, ny // 32, ybody, 0)
        chunk = 64

        def xbody(i, _):
            r = pl.ds(i * chunk, chunk)
            cols = col[r, :]
            across = lax.broadcasted_iota(jnp.int32, (chunk, nx), 1)
            cell = cols[:, 0:1].astype(jnp.int32)
            table = banded(across, cell, [cols[:, 1 + j : 2 + j] for j in range(4)], nx)
            xtab[r, :] = table.astype(jnp.bfloat16)
            xtab32[r, :] = table
            across = lax.broadcasted_iota(jnp.int32, (chunk, ny), 1)
            cell = cols[:, 5:6].astype(jnp.int32)
            y = banded(across, cell, [cols[:, 6 + j : 7 + j] for j in range(4)], ny)
            for z in range(layers):
                p = place[z] * ny
                slhs[r, p : p + ny] = (cols[:, 10 + z : 11 + z] * y).astype(jnp.bfloat16)
            return 0

        lax.fori_loop(0, both // chunk, xbody, 0)

    def spread(new, z):
        def lhs_body(i, _):
            y = ytab[pl.ds(i * 16, 16), :]
            for c in range(3):
                lhs[pl.ds(c * ny + i * 16, 16), :] = (rowg[z, c : c + 1, :] * y).astype(jnp.bfloat16)
            return 0

        lax.fori_loop(0, ny // 16, lhs_body, 0)
        force = jnp.dot(lhs[...], xtab[...], preferred_element_type=jnp.float32)
        for c in range(3):
            for b in range(nxb):
                vv[new, c, z, b, PAD : PAD + ny, :] += (
                    DT * force[c * ny : (c + 1) * ny, b * LANES : (b + 1) * LANES]
                )

    def lower_inner(new, final):
        def body(i, _):
            r = pl.ds(PAD + i * 16, 16)
            for z in inner:
                for c in range(3):
                    for b in range(nxb):
                        value = vv[new, c, z, b, r, :]
                        cut = slice(b * LANES, (b + 1) * LANES)
                        low[c, pl.ds(place[z] * ny + i * 16, 16), cut] = value.astype(jnp.bfloat16)
                        if final:
                            out_ref[c, z, pl.ds(i * 16, 16), cut] = value
            return 0

        lax.fori_loop(0, ny // 16, body, 0)

    def finish_edges(step, final, lo, hi):
        now, new = step % 2, 1 - step % 2

        def body(k, _):
            for side in range(2):
                halo_copy(step, 1 - side, k).wait_recv()
            for side, z in enumerate(edges):
                sign = (0.5 * DT, -0.5 * DT)[side]
                if final:
                    halo_copy(step, side, k).wait_send()
                for i in range(rows // 16):
                    y0 = k * rows + i * 16
                    for b in range(nxb):
                        cut = slice(b * LANES, (b + 1) * LANES)
                        factor = DT * VISC + sign * vv[now, 2, z, b, pl.ds(PAD + y0, 16), :]
                        for c in range(3):
                            value = vv[new, c, z, b, pl.ds(PAD + y0, 16), :] + factor * halo[
                                step, side, c, pl.ds(y0, 16), cut
                            ].astype(jnp.float32)
                            low[c, pl.ds(place[z] * ny + y0, 16), cut] = value.astype(jnp.bfloat16)
                            if final:
                                out_ref[c, z, pl.ds(y0, 16), cut] = value
                            else:
                                vv[new, c, z, b, pl.ds(PAD + y0, 16), :] = value
            if not final:
                for side in range(2):
                    halo_copy(step + 1, side, k).start()
            return 0

        lax.fori_loop(lo, hi, body, 0)

    def sample(first, final_part):
        depth = len(inner) * ny if first else len(edges) * ny
        base = 0 if first else len(inner) * ny

        def body(t, _):
            r = pl.ds(pl.multiple_of(t * 256, 256), 256)
            for c in range(3):
                lines = jnp.dot(
                    slhs[r, base : base + depth],
                    low[c, base : base + depth, :],
                    preferred_element_type=jnp.float32,
                )
                lines = lines * xtab32[r, :]
                total = lines[:, 0:LANES]
                for b in range(1, nxb):
                    total += lines[:, b * LANES : (b + 1) * LANES]
                if first:
                    acc[c, r, :] = total
                else:
                    acc[c, r, :] += total
            return 0

        lax.fori_loop(0, both // 256, body, 0)

    def parts(step):
        for part in range(2):
            r = slice(part * markers, (part + 1) * markers)
            sums = [jnp.sum(acc[c, r, :], axis=1, keepdims=True) for c in range(3)]
            zero = jnp.zeros((markers, 5), jnp.float32)
            partbuf[step, part] = jnp.concatenate(sums + [zero], axis=1).T

    def part_copy(step, part):
        return pltpu.make_async_remote_copy(
            partbuf.at[step, part],
            partin.at[step, part],
            ps_sem.at[step, part],
            pr_sem.at[step, part],
            device_id=((right, left)[part],),
            device_id_type=MESH,
        )

    for step in range(STEPS):
        now, new = step % 2, 1 - step % 2
        final = step == STEPS - 1
        wrap_rows(now)
        for z in edges + inner:
            stencil(now, z)
        if step == 0:
            marker_copy.wait()
        else:
            for part in range(2):
                part_copy(step - 1, part).wait()
        tables(step)
        for z in edges + inner:
            spread(new, z)
        finish_edges(step, final, 0, CHUNKS // 2)
        lower_inner(new, final)
        sample(True, False)
        finish_edges(step, final, CHUNKS // 2, CHUNKS)
        sample(False, final)
        parts(step)
        for part in range(1 if final else 0, 2):
            part_copy(step, part).start()
        if step == 0:
            for k in range(CHUNKS):
                for side in range(2):
                    halo_copy(0, side, k).wait_send()
    last = STEPS - 1
    part_copy(last, 1).wait()
    moved = partbuf[last, 0, 0:3, :] + partin[last, 1, 0:3, :]
    offout_ref[...] = own[0:3, :] + DT * (own[9:10, :] * moved)


def local(velocity, offsets, bases, targets, stiffness, active_block_count):
    _, layers, ny, nx = velocity.shape
    markers = offsets.shape[1]
    both = 2 * markers
    nxb = nx // LANES
    vmem = pl.BlockSpec(memory_space=pltpu.VMEM)
    hbm = pl.BlockSpec(memory_space=pl.ANY)
    smem = pl.BlockSpec(memory_space=pltpu.SMEM)
    f32, bf16 = jnp.float32, jnp.bfloat16
    dma = pltpu.SemaphoreType.DMA
    return pl.pallas_call(
        kernel,
        out_shape=[
            jax.ShapeDtypeStruct(velocity.shape, f32),
            jax.ShapeDtypeStruct(offsets.shape, f32),
        ],
        in_specs=[hbm, vmem, vmem, vmem, vmem, smem],
        out_specs=[vmem, vmem],
        scratch_shapes=[
            pltpu.VMEM((2, 3, layers, nxb, ny + 2 * PAD, LANES), f32),
            pltpu.VMEM((16, markers), f32),
            pltpu.VMEM((16, markers), f32),
            pltpu.VMEM((2, 3, ny, nx), bf16),
            pltpu.VMEM((STEPS, 2, 3, ny, nx), bf16),
            pltpu.VMEM((3, layers * ny, nx), bf16),
            pltpu.VMEM((3 * ny, both), bf16),
            pltpu.VMEM((both, nx), bf16),
            pltpu.VMEM((both, nx), f32),
            pltpu.VMEM((ny, both), f32),
            pltpu.VMEM((both, layers * ny), bf16),
            pltpu.VMEM((both, 16), f32),
            pltpu.VMEM((layers, 8, both), f32),
            pltpu.VMEM((3, both, LANES), f32),
            pltpu.VMEM((STEPS, 2, 8, markers), f32),
            pltpu.VMEM((STEPS, 2, 8, markers), f32),
            dma((layers, nxb)),
            dma((2,)),
            dma((STEPS, 2, CHUNKS)),
            dma((STEPS, 2, CHUNKS)),
            dma((STEPS, 2)),
            dma((STEPS, 2)),
        ],
        compiler_params=pltpu.CompilerParams(
            collective_id=0, has_side_effects=True, vmem_limit_bytes=60 * 1024 * 1024
        ),
        name="immersed_steps",
    )(velocity, offsets, bases, targets, stiffness.reshape(1, markers), active_block_count)


def solution(mesh):
    return jax.shard_map(
        local,
        mesh=mesh,
        in_specs=(
            P(None, "gz", None, None),
            P(None, "gz"),
            P(None, "gz"),
            P(None, "gz"),
            P("gz"),
            P("gz"),
        ),
        out_specs=(P(None, "gz", None, None), P(None, "gz")),
        check_vma=False,
    )
```

```python
import functools
import math

import jax
import jax.numpy as jnp
from jax import lax
from jax.experimental import pallas as pl
from jax.experimental.pallas import tpu as pltpu
from jax.sharding import PartitionSpec as P

BLK = 256
STEPS = 2
DT = 0.2
VISC = 0.3
LANES = 128
PAD = 8
CHUNKS = 8
STRIP = 32
EARLY = 2
MESH = pl.DeviceIdType.MESH


def weights_of(offsets):
    angle = (0.5 * math.pi) * offsets
    c, s = jnp.cos(angle), jnp.sin(angle)
    return [0.25 * (1.0 + c), 0.25 * (1.0 + s), 0.25 * (1.0 - c), 0.25 * (1.0 - s)]


def banded(across, cell, weights, extent):
    apart = across - cell
    if extent & (extent - 1) == 0:
        apart = apart & (extent - 1)
    else:
        apart = jnp.where(apart < 0, apart + extent, apart)
    table = jnp.where(apart == 3, weights[3], 0.0)
    for j in (2, 1, 0):
        table = jnp.where(apart == j, weights[j], table)
    return table


def plane_weights(level, weights_z, layers):
    planes = []
    for z in range(layers):
        row = jnp.zeros(level.shape, jnp.float32)
        for j in range(4):
            row = jnp.where(level + j == z, weights_z[j], row)
        planes.append(row)
    return planes


def kernel(
    v_hbm, off_hbm, base_hbm, tgt_hbm, stiff_hbm, cnt_ref,
    out_ref, corr_ref, elhs_ref, xown_ref, marks_ref,
    va, vb, ring, off_ref, base_ref, tgt_ref, stiff_ref, own, near, send, halo, lowt, lhs, xtab, xtab32,
    ytab, slhs, rowg, wrow, irow, sums, partin, arg_sem, in_sem, mk_sem, hs_sem, hr_sem, ps_sem, pr_sem,
):
    _, layers, nxb, nyp, _ = va.shape
    vv = (va, vb)
    ny = nyp - 2 * PAD
    nx = nxb * LANES
    markers = own.shape[1]
    both = 2 * markers
    rows = ny // CHUNKS
    me = lax.axis_index("gz")
    count = lax.axis_size("gz")
    right = lax.rem(me + 1, count)
    left = lax.rem(me + count - 1, count)
    edges = (0, layers - 1)
    inner = tuple(range(1, layers - 1))
    order = inner + edges
    place = {z: i for i, z in enumerate(order)}

    barrier = pltpu.get_barrier_semaphore()
    for neighbour in (left, right):
        pl.semaphore_signal(barrier, inc=1, device_id=(neighbour,), device_id_type=MESH)

    args = [
        pltpu.make_async_copy(source, target, arg_sem.at[i])
        for i, (source, target) in enumerate(
            ((off_hbm, off_ref), (base_hbm, base_ref), (tgt_hbm, tgt_ref), (stiff_hbm, stiff_ref))
        )
    ]
    for copy in args:
        copy.start()

    def load(z, b):
        return pltpu.make_async_copy(
            v_hbm.at[:, z, :, pl.ds(b * LANES, LANES)],
            va.at[:, z, b, pl.ds(PAD, ny), :],
            in_sem.at[z, b],
        )

    for z in edges + inner:
        for b in range(nxb):
            load(z, b).start()

    for copy in args:
        copy.wait()
    living = (
        lax.broadcasted_iota(jnp.int32, (1, markers), 1) // BLK < cnt_ref[0]
    ).astype(jnp.float32)
    own[0:3, :] = off_ref[...]
    own[3:5, :] = base_ref[0:2, :].astype(jnp.float32)
    own[5:6, :] = (base_ref[2:3, :] - me * layers).astype(jnp.float32)
    own[6:9, :] = tgt_ref[...]
    own[9:10, :] = living
    own[10:11, :] = living * stiff_ref[...]
    own[11:16, :] = jnp.zeros((5, markers), jnp.float32)

    pl.semaphore_wait(barrier, 2)
    marker_copy = pltpu.make_async_remote_copy(
        own, near, mk_sem.at[0], mk_sem.at[1], device_id=(right,), device_id_type=MESH
    )
    marker_copy.start()

    def halo_copy(step, side, k):
        r = pl.ds(k * rows, rows)
        return pltpu.make_async_remote_copy(
            send.at[step, side, :, r],
            halo.at[step, 1 - side, :, r],
            hs_sem.at[step, side, k],
            hr_sem.at[step, 1 - side, k],
            device_id=((left, right)[side],),
            device_id_type=MESH,
        )

    for z in edges:
        for b in range(nxb):
            load(z, b).wait()

    def cast_chunk(k, _):
        for side, z in enumerate(edges):
            for c in range(3):
                for b in range(nxb):
                    send[0, side, c, pl.ds(k * rows, rows), b * LANES : (b + 1) * LANES] = va[
                        c, z, b, pl.ds(PAD + k * rows, rows), :
                    ].astype(jnp.bfloat16)
        for side in range(2):
            halo_copy(0, side, k).start()
        return 0

    lax.fori_loop(0, CHUNKS, cast_chunk, 0)
    for z in inner:
        for b in range(nxb):
            load(z, b).wait()

    def wrap_rows(v):
        for c in range(3):
            for z in range(layers):
                for b in range(nxb):
                    v[c, z, b, PAD - 1 : PAD, :] = v[c, z, b, PAD + ny - 1 : PAD + ny, :]
                    v[c, z, b, PAD + ny : PAD + ny + 1, :] = v[c, z, b, PAD : PAD + 1, :]

    def shift_block(old, z, y0):
        lane = lax.broadcasted_iota(jnp.int32, (8, LANES), 1)
        first, last = lane == 0, lane == LANES - 1
        for j in range(STRIP // 8):
            for c in range(3):
                here = [old[c, z, b, pl.ds(y0 + 8 * j, 8), :] for b in range(nxb)]
                fore = [pltpu.roll(h, LANES - 1, 1) for h in here]
                back = [pltpu.roll(h, 1, 1) for h in here]
                for b in range(nxb):
                    r = slice(8 * j, 8 * j + 8)
                    ring[0, c, b, r, :] = jnp.where(last, fore[(b + 1) % nxb], fore[b])
                    ring[1, c, b, r, :] = jnp.where(first, back[(b - 1) % nxb], back[b])

    def stencil(old, new, z, after):
        steps = ny // STRIP

        def body(i, _):
            base = PAD + i * STRIP
            for j in range(STRIP // 8):
                y0 = base + 8 * j
                r = slice(8 * j, 8 * j + 8)
                for b in range(nxb):
                    here = [old[c, z, b, pl.ds(y0, 8), :] for c in range(3)]
                    half = [(0.5 * DT) * h for h in here]
                    up = [DT * VISC - h for h in half]
                    down = [DT * VISC + h for h in half]
                    for c in range(3):
                        total = (1.0 - 6.0 * DT * VISC) * here[c]
                        total += up[1] * old[c, z, b, pl.ds(y0 + 1, 8), :]
                        total += down[1] * old[c, z, b, pl.ds(y0 - 1, 8), :]
                        if z < layers - 1:
                            total += up[2] * old[c, z + 1, b, pl.ds(y0, 8), :]
                        if z > 0:
                            total += down[2] * old[c, z - 1, b, pl.ds(y0, 8), :]
                        total += up[0] * ring[0, c, b, r, :]
                        total += down[0] * ring[1, c, b, r, :]
                        new[c, z, b, pl.ds(y0, 8), :] = total
            done = i == steps - 1
            shift_block(old, jnp.where(done, after, z), jnp.where(done, PAD, base + STRIP))
            return 0

        lax.fori_loop(0, steps, body, 0)

    def tables(step, final):
        halves = []
        for i, ref in enumerate((own, near)):
            info = ref[...]
            offsets = info[0:3]
            if step > 0:
                if i == 0:
                    moved = sums[step - 1, 0, 0:3, :] + partin[step - 1, 1, 0:3, :]
                else:
                    moved = partin[step - 1, 0, 0:3, :] + sums[step - 1, 1, 0:3, :]
                offsets = offsets + DT * (info[9:10] * moved)
                ref[0:3, :] = offsets
            level = info[5:6] - float(i * layers)
            forces = info[10:11] * (info[6:9] - offsets)
            halves.append((offsets, info[3:5].astype(jnp.int32), level.astype(jnp.int32), forces))
        offsets, cells, level, forces = [jnp.concatenate(p, axis=1) for p in zip(*halves)]
        weights = weights_of(offsets)
        planes = plane_weights(level, [w[2:3] for w in weights], layers + 1)
        for z in range(layers):
            for c in range(3):
                rowg[z, c : c + 1, :] = forces[c : c + 1] * planes[z]
        irow[0:2, :] = cells[0:2]
        for a in range(2):
            for j in range(4):
                wrow[4 * a + j : 4 * a + j + 1, :] = weights[j][a : a + 1]
        for z in range(layers + 1):
            wrow[8 + z : 9 + z, :] = planes[z]
        tile, block = 256, 64

        def table_of(a, i, m, extent):
            across = lax.broadcasted_iota(jnp.int32, (block, tile), 0) + i * block
            w = [wrow[4 * a + j : 4 * a + j + 1, m] for j in range(4)]
            return banded(across, irow[a : a + 1, m], w, extent)

        for part in range(2):
            tiles = markers // tile

            def ybody(n, _):
                t, i = n % tiles, n // tiles
                r = pl.ds(pl.multiple_of(i * block, block), block)
                w = pl.ds(pl.multiple_of(t * tile, tile), tile)
                m = pl.ds(pl.multiple_of(part * markers + t * tile, tile), tile)
                table = table_of(1, i, m, ny)
                ytab[r, m] = table
                for z in range(layers):
                    if part == 1 and z > 2:
                        continue
                    plane = (wrow[8 + z : 9 + z, m] * table).astype(jnp.bfloat16)
                    slhs[pl.ds(place[z] * ny + i * block, block), m] = plane
                    if final and part == 0 and z in edges:
                        elhs_ref[pl.ds(edges.index(z) * ny + i * block, block), w] = plane
                if final and part == 0:
                    plane = wrow[8 + layers : 9 + layers, m] * table
                    elhs_ref[pl.ds(2 * ny + i * block, block), w] = plane.astype(jnp.bfloat16)
                return 0

            lax.fori_loop(0, tiles * (ny // block), ybody, 0)

            def xbody(n, _):
                t, i = n % tiles, n // tiles
                r = pl.ds(pl.multiple_of(i * block, block), block)
                w = pl.ds(pl.multiple_of(t * tile, tile), tile)
                m = pl.ds(pl.multiple_of(part * markers + t * tile, tile), tile)
                table = table_of(0, i, m, nx)
                xtab[r, m] = table.astype(jnp.bfloat16)
                xtab32[r, m] = table
                if final and part == 0:
                    xown_ref[r, w] = table
                return 0

            lax.fori_loop(0, tiles * (nx // block), xbody, 0)

    def spread(new, z, final):
        reach = both if z <= 2 else markers

        def lhs_body(i, _):
            y = ytab[pl.ds(i * 16, 16), :reach]
            for c in range(3):
                product = rowg[z, c : c + 1, :reach] * y
                lhs[pl.ds(c * ny + i * 16, 16), :reach] = product.astype(jnp.bfloat16)
            return 0

        lax.fori_loop(0, ny // 16, lhs_body, 0)
        force = lax.dot_general(
            lhs[:, :reach], xtab[:, :reach], (((1,), (1,)), ((), ())), preferred_element_type=jnp.float32
        )
        for c in range(3):
            for b in range(nxb):
                cut = slice(b * LANES, (b + 1) * LANES)
                value = new[c, z, b, PAD : PAD + ny, :] + DT * force[c * ny : (c + 1) * ny, cut]
                if final and z in inner:
                    out_ref[c, z, :, cut] = value
                else:
                    new[c, z, b, PAD : PAD + ny, :] = value

    def lower(new, planes, final):
        def body(c, _):
            for z in planes:
                for b in range(nxb):
                    cut = slice(b * LANES, (b + 1) * LANES)
                    if final and z in inner:
                        value = out_ref[c, z, :, cut]
                    else:
                        value = new[c, z, b, PAD : PAD + ny, :]
                    lowt[c, cut, place[z] * ny : (place[z] + 1) * ny] = value.astype(jnp.bfloat16).T
            return 0

        lax.fori_loop(0, 3, body, 0)

    def finish_edges(step, final, lo, hi, post=False):
        old, new = vv[step % 2], vv[1 - step % 2]
        cell = DT * VISC

        def body(k, _):
            for side in range(2):
                halo_copy(step, 1 - side, k).wait_recv()
            for i in range(rows // 16):
                y0 = k * rows + i * 16
                r = pl.ds(y0, 16)
                v = pl.ds(PAD + y0, 16)
                for b in range(nxb):
                    cut = slice(b * LANES, (b + 1) * LANES)
                    for side, z in enumerate(edges):
                        sign = (0.5 * DT, -0.5 * DT)[side]
                        outer = [halo[step, side, c, r, cut].astype(jnp.float32) for c in range(3)]
                        factor = cell + sign * old[2, z, b, v, :]
                        for c in range(3):
                            change = factor * outer[c]
                            value = new[c, z, b, v, :] + change
                            if final:
                                out_ref[c, z, r, cut] = value
                                corr_ref[side, c, r, cut] = change.astype(jnp.bfloat16)
                            else:
                                new[c, z, b, v, :] = value
                                send[step + 1, side, c, r, cut] = value.astype(jnp.bfloat16)
                        if final and side == 1:
                            beyond = cell + (0.5 * DT) * outer[2]
                            for c in range(3):
                                corr_ref[2, c, r, cut] = (beyond * old[c, z, b, v, :]).astype(jnp.bfloat16)
            if post:
                post_chunk(step + 1, k)
            return 0

        lax.fori_loop(lo, hi, body, 0)

    def post_chunk(step, k):
        for side in range(2):
            halo_copy(step, side, k).start()

    def sample(step, planes, first):
        base = place[planes[0]] * ny
        tile = 256

        for part in range(2):
            depth = len([z for z in planes if part == 0 or z <= 2]) * ny

            def body(t, _):
                m = pl.ds(pl.multiple_of(part * markers + t * tile, tile), tile)
                w = pl.ds(pl.multiple_of(t * tile, tile), tile)
                for c in range(3):
                    lines = jnp.dot(
                        lowt[c, :, base : base + depth],
                        slhs[base : base + depth, m],
                        preferred_element_type=jnp.float32,
                    )
                    total = jnp.sum(lines * xtab32[:, m], axis=0, keepdims=True)
                    if first:
                        sums[step, part, c : c + 1, w] = total
                    else:
                        sums[step, part, c : c + 1, w] += total
                return 0

            lax.fori_loop(0, markers // tile, body, 0)

    def part_copy(step, part):
        return pltpu.make_async_remote_copy(
            sums.at[step, part],
            partin.at[step, part],
            ps_sem.at[step, part],
            pr_sem.at[step, part],
            device_id=((right, left)[part],),
            device_id_type=MESH,
        )

    sums[...] = jnp.zeros_like(sums)
    for step in range(STEPS):
        old, new = vv[step % 2], vv[1 - step % 2]
        final = step == STEPS - 1
        wrap_rows(old)
        sweep = edges + inner
        shift_block(old, sweep[0], PAD)

        def stencils(planes):
            for z in planes:
                i = sweep.index(z)
                stencil(old, new, z, sweep[(i + 1) % layers])

        stencils(edges)
        if step == 0:
            marker_copy.wait()
        else:
            stencils(inner)
            for part in range(2):
                part_copy(step - 1, part).wait()
        tables(step, final)
        for z in edges:
            spread(new, z, final)
        if final:
            for z in inner:
                spread(new, z, final)
            lower(new, order, True)
            sample(step, order, True)
            part_copy(step, 1).start()
            finish_edges(step, True, 0, CHUNKS)
        else:
            finish_edges(step, False, 0, EARLY, True)
            stencils(inner)
            for z in inner:
                spread(new, z, final)
            lower(new, inner, False)
            sample(step, inner, True)
            finish_edges(step, False, EARLY, CHUNKS)
            lower(new, edges, False)
            sample(step, edges, False)
            for part in range(2):
                part_copy(step, part).start()
            for k in range(EARLY, CHUNKS):
                post_chunk(step + 1, k)
    last = STEPS - 1
    part_copy(last, 1).wait()
    marks_ref[0:3, :] = own[0:3, :]
    marks_ref[3:6, :] = sums[last, 0, 0:3, :] + partin[last, 1, 0:3, :]
    marks_ref[6:7, :] = own[9:10, :]
    marks_ref[7:8, :] = jnp.zeros((1, markers), jnp.float32)
    for step in range(STEPS):
        for k in range(CHUNKS):
            for side in range(2):
                halo_copy(step, side, k).wait_send()


def closing_kernel(v_ref, corr_ref, elhs_ref, x_ref, marks_ref, v_hbm, off_ref, cornt, sem):
    comps, layers, ny, nx = v_ref.shape
    copies = []
    for z in range(layers):
        for c in range(comps):
            copies.append(pltpu.make_async_copy(v_ref.at[c, z], v_hbm.at[c, z], sem.at[c, z]))
    for copy in copies:
        copy.start()
    for c in range(comps):
        for p in range(corr_ref.shape[0]):
            for b in range(nx // LANES):
                cut = slice(b * LANES, (b + 1) * LANES)
                cornt[c, cut, p * ny : (p + 1) * ny] = corr_ref[p, c, :, cut].T
        lines = jnp.dot(cornt[c], elhs_ref[...], preferred_element_type=jnp.float32)
        total = jnp.sum(lines * x_ref[...], axis=0, keepdims=True)
        off_ref[c : c + 1, :] = marks_ref[c : c + 1, :] + DT * (
            marks_ref[6:7, :] * (marks_ref[3 + c : 4 + c, :] + total)
        )
    for copy in copies:
        copy.wait()


def local(velocity, offsets, bases, targets, stiffness, active_block_count):
    _, layers, ny, nx = velocity.shape
    markers = offsets.shape[1]
    both = 2 * markers
    nxb = nx // LANES
    vmem = pl.BlockSpec(memory_space=pltpu.VMEM)
    hbm = pl.BlockSpec(memory_space=pl.ANY)
    smem = pl.BlockSpec(memory_space=pltpu.SMEM)
    f32, bf16 = jnp.float32, jnp.bfloat16
    dma = pltpu.SemaphoreType.DMA
    field = pltpu.VMEM((3, layers, nxb, ny + 2 * PAD, LANES), f32)
    results = pl.pallas_call(
        kernel,
        out_shape=[
            jax.ShapeDtypeStruct(velocity.shape, f32),
            jax.ShapeDtypeStruct((3, 3, ny, nx), bf16),
            jax.ShapeDtypeStruct((3 * ny, markers), bf16),
            jax.ShapeDtypeStruct((nx, markers), f32),
            jax.ShapeDtypeStruct((8, markers), f32),
        ],
        in_specs=[pl.BlockSpec(memory_space=pltpu.HBM)] * 5 + [smem],
        out_specs=[vmem] * 5,
        scratch_shapes=[
            field,
            field,
            pltpu.VMEM((2, 3, nxb, STRIP, LANES), f32),
            pltpu.VMEM((3, markers), f32),
            pltpu.VMEM((3, markers), jnp.int32),
            pltpu.VMEM((3, markers), f32),
            pltpu.VMEM((1, markers), f32),
            pltpu.VMEM((16, markers), f32),
            pltpu.VMEM((16, markers), f32),
            pltpu.VMEM((STEPS, 2, 3, ny, nx), bf16),
            pltpu.VMEM((STEPS, 2, 3, ny, nx), bf16),
            pltpu.VMEM((3, nx, layers * ny), bf16),
            pltpu.VMEM((3 * ny, both), bf16),
            pltpu.VMEM((nx, both), bf16),
            pltpu.VMEM((nx, both), f32),
            pltpu.VMEM((ny, both), f32),
            pltpu.VMEM((layers * ny, both), bf16),
            pltpu.VMEM((layers, 8, both), f32),
            pltpu.VMEM((16, both), f32),
            pltpu.VMEM((8, both), jnp.int32),
            pltpu.VMEM((STEPS, 2, 8, markers), f32),
            pltpu.VMEM((STEPS, 2, 8, markers), f32),
            dma((4,)),
            dma((layers, nxb)),
            dma((2,)),
            dma((STEPS, 2, CHUNKS)),
            dma((STEPS, 2, CHUNKS)),
            dma((STEPS, 2)),
            dma((STEPS, 2)),
        ],
        compiler_params=pltpu.CompilerParams(
            collective_id=0, has_side_effects=True, vmem_limit_bytes=40 * 1024 * 1024
        ),
        name="immersed_steps",
    )(
        velocity,
        *[
            pltpu.with_memory_space_constraint(a, pltpu.HBM)
            for a in (offsets, bases, targets, stiffness.reshape(1, markers))
        ],
        active_block_count,
    )
    return pl.pallas_call(
        closing_kernel,
        out_shape=[
            jax.ShapeDtypeStruct(velocity.shape, f32),
            jax.ShapeDtypeStruct(offsets.shape, f32),
        ],
        in_specs=[vmem] * 5,
        out_specs=[hbm, vmem],
        scratch_shapes=[pltpu.VMEM((3, nx, 3 * ny), bf16), dma((3, layers))],
        compiler_params=pltpu.CompilerParams(vmem_limit_bytes=16 * 1024 * 1024),
        name="closing",
    )(*results)


def solution(mesh):
    return jax.shard_map(
        local,
        mesh=mesh,
        in_specs=(
            P(None, "gz", None, None),
            P(None, "gz"),
            P(None, "gz"),
            P(None, "gz"),
            P("gz"),
            P("gz"),
        ),
        out_specs=(P(None, "gz", None, None), P(None, "gz")),
        check_vma=False,
    )
```
